32 devices in a mesh: expert: 4 (over z), tensor: 8 (over y, x, core).
Axes of the slice: x: 2, y: 2, z: 4, core: 2. Of those that a mesh axis runs over, the one named last changes fastest.
Arguments:
- expert_inputs: bfloat16 [8, 64, 4096], P('expert'), may hold values from -6 to 6
- gates: float32 [8, 64], P('expert'), may hold values from 0.2 to 1
- chosen_tokens: int32 [8, 64], replicated, may hold values from 0 to 4095, as said below
- w_gate: bfloat16 [8, 4096, 1792], P('expert', None, 'tensor'), may hold values from -0.09375 to 0.09375
- w_up: bfloat16 [8, 4096, 1792], P('expert', None, 'tensor'), may hold values from -0.09375 to 0.09375
- w_down: bfloat16 [8, 1792, 4096], P('expert', 'tensor'), may hold values from -0.125 to 0.125
- residual: bfloat16 [4096, 4096], P(('expert', 'tensor')), may hold values from -6 to 6
- norm_gain: float32 [4096], replicated, may hold values from 0.5 to 1.5
- w_qkv: bfloat16 [4096, 12288], P(None, 'tensor'), may hold values from -0.09375 to 0.09375
Outputs:
- stream: bfloat16 [4096, 4096], P(('expert', 'tensor'))
- projected: bfloat16 [4096, 12288], P('expert', 'tensor')
The draws below stay inside these ranges and needn't reach their ends.
Inputs may be any that keep to these rules, and one draw needn't show every extreme that they name: `chosen_tokens`: each row holds 64 different token indices; at most 4 of a row lie in one block of 128 consecutive tokens, and in every draw some block holds 4 tokens of every row.
All inputs are finite; a program needn't handle non-finite values.
Results may differ from the reference program's by a relative error of at most 0.005.
Values may be sent and summed in bfloat16 or wider, within the bound.
No kernel may reach another device: no remote copies, remote signals or barrier semaphores. Data moves between devices by JAX's collectives and lax.ppermute only.
A program may use at most 128 MiB of HBM per device.

```python
import jax
import jax.numpy as jnp
from jax import lax

D = 4096
FF = 1792
TOK_DEV = 128
MOST = 4
EXPERTS_LIVE = 8
CAP = 64
TOKENS = 4096


def draw_chosen_tokens(key, part):
    owner_total = TOKENS // TOK_DEV
    key_hot, key_forced, key_score, key_base = jax.random.split(jax.random.fold_in(key, 17), 4)
    popularity = jax.random.randint(key_hot, (owner_total,), 0, 4)
    mandatory_pick = jax.random.randint(key_forced, (), 0, owner_total)
    holder_numbers = jnp.arange(owner_total, dtype=jnp.int32)
    extra_score = popularity * 16384 + jnp.where(holder_numbers == mandatory_pick, 262144, 0)
    noise_term = jax.random.randint(key_score, (EXPERTS_LIVE, owner_total, MOST), 0, 65536)
    affinity_scores = noise_term + extra_score[None, :, None]
    ticket_ids = jnp.arange(owner_total * MOST, dtype=jnp.int32).reshape(1, owner_total, MOST)
    distinct = (affinity_scores * (owner_total * MOST) + ticket_ids).reshape(EXPERTS_LIVE, owner_total * MOST)
    picked_scores, picked = jax.lax.top_k(distinct, CAP)
    picked_owner = picked // MOST
    picked_rank = picked % MOST
    base_offset = jax.random.randint(key_base, (EXPERTS_LIVE, owner_total), 0, TOK_DEV)
    chosen_base = jnp.take_along_axis(base_offset, picked_owner, axis=1)
    offsets = (chosen_base + picked_rank) % TOK_DEV
    return (picked_owner * TOK_DEV + offsets).astype(jnp.int32)


def level_of(key, shape, shards, smallest, top_value):
    loudness, own = 1.0, jax.random.fold_in(key, 6)
    for axis_at, parts in shards:
        heights = jnp.exp(jax.random.uniform(jax.random.fold_in(own, axis_at), (parts,), jnp.float32, smallest / len(shards), top_value / len(shards)))
        loudness = loudness * jnp.repeat(heights, shape[axis_at] // parts).reshape([-1 if axis == axis_at else 1 for axis in range(len(shape))])
    return loudness


def normal_values(rng, extent, spread, most, cuts=(), held_as=jnp.bfloat16):
    entries = spread * jax.random.normal(rng, extent, jnp.float32)
    if cuts:
        entries = entries * level_of(rng, extent, cuts, -0.22, 0.18)
    return jnp.clip(entries, -most, most).astype(held_as)


def setup_inputs(seed: int = 0) -> dict:
    streams_of = jax.random.split(jax.random.key(seed), 10)
    expert_inputs = normal_values(streams_of[0], (EXPERTS_LIVE, CAP, D), 1.0, 6.0, ((0, 4),))
    gates = jnp.clip(0.2 + 0.8 * jax.random.uniform(streams_of[1], (EXPERTS_LIVE, CAP), jnp.float32) ** level_of(streams_of[1], (EXPERTS_LIVE, CAP), ((0, 4),), -0.2, 0.2), 0.2, 1.0)
    chosen_tokens = draw_chosen_tokens(jax.random.fold_in(streams_of[9], 71), 0)
    w_gate = normal_values(streams_of[3], (EXPERTS_LIVE, D, FF), D ** -0.5, 0.09375, ((0, 4), (2, 8)))
    w_up = normal_values(streams_of[4], (EXPERTS_LIVE, D, FF), D ** -0.5, 0.09375, ((0, 4), (2, 8)))
    w_down = normal_values(streams_of[5], (EXPERTS_LIVE, FF, D), FF ** -0.5, 0.125, ((0, 4), (1, 8)))
    residual = normal_values(streams_of[6], (TOKENS, D), 1.0, 6.0, ((0, 32),))
    norm_gain = jnp.clip(1.0 + 0.1 * jax.random.normal(streams_of[7], (D,), jnp.float32), 0.5, 1.5)
    w_qkv = normal_values(streams_of[8], (D, 3 * D), D ** -0.5, 0.09375, ((1, 8),))
    return {"expert_inputs": expert_inputs, "gates": gates, "chosen_tokens": chosen_tokens, "w_gate": w_gate, "w_up": w_up, "w_down": w_down, "residual": residual, "norm_gain": norm_gain, "w_qkv": w_qkv}


def expert_apply(operands):
    inputs_block, gate_block, gate_weight, up_weight, down_weight = operands
    gate_part = jnp.dot(inputs_block, gate_weight, preferred_element_type=jnp.float32)
    up_part = jnp.dot(inputs_block, up_weight, preferred_element_type=jnp.float32)
    hidden = (jax.nn.silu(gate_part) * up_part).astype(jnp.bfloat16)
    return jnp.dot(hidden, down_weight, preferred_element_type=jnp.float32) * gate_block[:, None]

def reference(expert_inputs, gates, chosen_tokens, w_gate, w_up, w_down, residual, norm_gain, w_qkv):
    expert_out = lax.map(expert_apply, (expert_inputs, gates, w_gate, w_up, w_down))
    scattered = jnp.zeros((TOKENS, D), jnp.float32).at[chosen_tokens.reshape(-1)].add(expert_out.reshape(-1, D))
    combined = residual.astype(jnp.float32) + scattered
    stream = combined.astype(jnp.bfloat16)
    scale_rows = lax.rsqrt(lax.optimization_barrier(jnp.mean(combined * combined, axis=-1, keepdims=True)) + 1e-06)
    normed = (combined * scale_rows * norm_gain[None, :]).astype(jnp.bfloat16)
    projected = jnp.dot(normed, w_qkv, preferred_element_type=jnp.float32).astype(jnp.bfloat16)
    return (stream, projected)
```

```python
import jax
import jax.numpy as jnp
from jax import lax
from jax.experimental import pallas as pl
from jax.experimental.pallas import tpu as pltpu
from jax.sharding import PartitionSpec as P


MOST = 4
CHUNKS = 4


def column_tile(columns):
    for tile in (512, 384, 256, 128):
        if columns % tile == 0:
            return tile
    return columns


def stream_kernel(rows, base, slots, contributions, out):
    row_total = rows.shape[0]
    token = base[0] + lax.broadcasted_iota(jnp.int32, (row_total, slots.shape[1]), 0)
    table = (token == slots[...]).astype(jnp.bfloat16)
    added = jnp.dot(table, contributions[0], preferred_element_type=jnp.float32)
    out[...] = (rows[...].astype(jnp.float32) + added).astype(jnp.bfloat16)


def make_stream(residual, base, token_of_slot, contributions):
    blocks, slots, part = contributions.shape
    row_total, width = residual.shape
    return pl.pallas_call(
        stream_kernel,
        grid=(blocks,),
        in_specs=[
            pl.BlockSpec((row_total, part), lambda t: (0, t)),
            pl.BlockSpec(memory_space=pltpu.SMEM),
            pl.BlockSpec((1, slots), lambda t: (0, 0)),
            pl.BlockSpec((1, slots, part), lambda t: (t, 0, 0)),
        ],
        out_specs=pl.BlockSpec((row_total, part), lambda t: (0, t)),
        out_shape=jax.ShapeDtypeStruct((row_total, width), jnp.bfloat16),
        cost_estimate=pl.CostEstimate(
            flops=2 * row_total * slots * width, bytes_accessed=4 << 20, transcendentals=0
        ),
        name="stream_rows",
    )(residual, base, token_of_slot, contributions)


def project_chunk(chunk, tok_rows, rows, token_of_slot, contributions, gain, weights, target):
    blocks, slots, part = contributions.shape
    row_total, width = rows.shape
    chunk_rows = row_total // blocks
    columns = weights.shape[1]
    tile = column_tile(columns)

    def kernel(rows_ref, slots_ref, contributions_ref, gain_ref, weights_ref, *rest):
        out, combined, normed = rest[-3:]

        @pl.when(pl.program_id(0) == 0)
        def _():
            row = lax.broadcasted_iota(jnp.int32, (row_total, slots), 0)
            token = (row // chunk_rows) * tok_rows + chunk * chunk_rows + row % chunk_rows
            table = (token == slots_ref[...]).astype(jnp.bfloat16)
            squares = jnp.zeros((row_total, 1), jnp.float32)
            for t in range(blocks):
                at = slice(t * part, (t + 1) * part)
                value = rows_ref[:, at].astype(jnp.float32) + jnp.dot(
                    table, contributions_ref[t], preferred_element_type=jnp.float32
                )
                combined[:, at] = value
                squares = squares + jnp.sum(value * value, axis=1, keepdims=True)
            scale = lax.rsqrt(squares / width + 1e-06)
            for t in range(blocks):
                at = slice(t * part, (t + 1) * part)
                normed[:, at] = (combined[:, at] * scale * gain_ref[:, at]).astype(jnp.bfloat16)

        value = jnp.dot(normed[...], weights_ref[...], preferred_element_type=jnp.float32)
        out[...] = value.astype(jnp.bfloat16).reshape(blocks, chunk_rows, tile)

    in_specs = [
        pl.BlockSpec((row_total, width), lambda n: (0, 0)),
        pl.BlockSpec((1, slots), lambda n: (0, 0)),
        pl.BlockSpec((blocks, slots, part), lambda n: (0, 0, 0)),
        pl.BlockSpec((1, width), lambda n: (0, 0)),
        pl.BlockSpec((width, tile), lambda n: (0, n)),
    ]
    operands = [rows, token_of_slot, contributions, gain, weights]
    aliases = {}
    if target is not None:
        in_specs.append(pl.BlockSpec(memory_space=pl.ANY))
        operands.append(target)
        aliases = {5: 0}
    return pl.pallas_call(
        kernel,
        grid=(columns // tile,),
        in_specs=in_specs,
        out_specs=pl.BlockSpec((blocks, chunk_rows, tile), lambda n: (0, chunk, n)),
        out_shape=jax.ShapeDtypeStruct((blocks, tok_rows, columns), jnp.bfloat16),
        scratch_shapes=[
            pltpu.VMEM((row_total, width), jnp.float32),
            pltpu.VMEM((row_total, width), jnp.bfloat16),
        ],
        input_output_aliases=aliases,
        cost_estimate=pl.CostEstimate(
            flops=2 * row_total * width * (columns + slots),
            bytes_accessed=2 * width * columns,
            transcendentals=0,
        ),
        compiler_params=pltpu.CompilerParams(vmem_limit_bytes=58 << 20),
        name="project_rows",
    )(*operands)


def layer(
    expert_inputs, gates, chosen_tokens, w_gate, w_up, w_down, residual, norm_gain, w_qkv
):
    expert_count = lax.axis_size("expert")
    tensor_count = lax.axis_size("tensor")
    group_index = lax.axis_index("expert")
    tensor_index = lax.axis_index("tensor")
    local_experts, slot_count, feature_width = expert_inputs.shape
    tok_rows = residual.shape[0]
    group_rows = tok_rows * tensor_count
    total_experts = expert_count * local_experts
    local_rows = local_experts * slot_count
    feature_part = feature_width // tensor_count
    chunk_rows = tok_rows // CHUNKS

    gathered = []
    for c in range(CHUNKS):
        piece = residual[c * chunk_rows : (c + 1) * chunk_rows]
        gathered.append(lax.all_gather(piece, "tensor", axis=0, tiled=True))

    in_group = (chosen_tokens // group_rows) == group_index
    rank = jnp.cumsum(in_group.astype(jnp.int32), axis=1) - 1
    per_expert = min(MOST * tensor_count, slot_count)
    compact_rows = total_experts * per_expert
    slot = jnp.where(
        in_group,
        jnp.arange(total_experts, dtype=jnp.int32)[:, None] * per_expert + rank,
        compact_rows,
    ).reshape(-1)
    pick = jnp.arange(compact_rows, dtype=jnp.int32)[:, None] == slot[None, :]
    local_token = (chosen_tokens % group_rows).reshape(-1)
    token_of_slot = jnp.sum(jnp.where(pick, local_token[None, :] + 1, 0), axis=1) - 1
    pick = pick.astype(jnp.bfloat16)

    gate_part = jnp.einsum(
        "ecd,edf->ecf", expert_inputs, w_gate, preferred_element_type=jnp.float32
    )
    up_part = jnp.einsum("ecd,edf->ecf", expert_inputs, w_up, preferred_element_type=jnp.float32)
    hidden = (jax.nn.silu(gate_part) * up_part).astype(jnp.bfloat16)
    partial_value = (
        jnp.einsum("ecf,efd->ecd", hidden, w_down, preferred_element_type=jnp.float32)
        * gates[:, :, None]
    ).astype(jnp.bfloat16)
    partial_rows = partial_value.reshape(local_rows, feature_width)

    blocks = lax.all_to_all(
        partial_rows, "tensor", split_axis=1, concat_axis=0, tiled=True
    ).reshape(tensor_count, local_rows, feature_part)
    summed = lax.optimization_barrier(jnp.sum(blocks.astype(jnp.float32), axis=0))
    every_row = lax.all_gather(summed.astype(jnp.bfloat16), "expert", axis=0, tiled=True)
    compact = jnp.dot(pick, every_row, preferred_element_type=jnp.float32).astype(jnp.bfloat16)
    contributions = lax.all_gather(compact, "tensor", axis=0, tiled=False)

    base = (tensor_index * tok_rows).astype(jnp.int32).reshape(1)
    slots = token_of_slot.reshape(1, compact_rows)
    gain = norm_gain.reshape(1, feature_width)
    stream = make_stream(residual, base, slots, contributions)
    projected = None
    for c in range(CHUNKS):
        projected = project_chunk(
            c, tok_rows, gathered[c], slots, contributions, gain, w_qkv, projected
        )
    return (stream, projected.reshape(group_rows, -1))


def solution(mesh):
    return jax.shard_map(
        layer,
        mesh=mesh,
        in_specs=(
            P("expert", None, None),
            P("expert", None),
            P(),
            P("expert", None, "tensor"),
            P("expert", None, "tensor"),
            P("expert", "tensor", None),
            P(("expert", "tensor"), None),
            P(),
            P(None, "tensor"),
        ),
        out_specs=(P(("expert", "tensor"), None), P("expert", "tensor")),
        check_vma=False,
    )
```

```python
import jax
import jax.numpy as jnp
from jax import lax
from jax.experimental import pallas as pl
from jax.experimental.pallas import tpu as pltpu
from jax.sharding import PartitionSpec as P


MOST = 4


def column_tile(columns):
    for tile in (512, 384, 256, 128):
        if columns % tile == 0:
            return tile
    return columns


def stream_kernel(place, rows, slots, contributions, out):
    row_total = rows.shape[0]
    token = place[0] * row_total + lax.broadcasted_iota(
        jnp.int32, (row_total, slots.shape[1]), 0
    )
    table = (token == slots[...]).astype(jnp.bfloat16)
    added = jnp.dot(table, contributions[0], preferred_element_type=jnp.float32)
    out[...] = (rows[...].astype(jnp.float32) + added).astype(jnp.bfloat16)


def make_stream(residual, place, token_of_slot, contributions):
    blocks, slots, part = contributions.shape
    row_total, width = residual.shape
    return pl.pallas_call(
        stream_kernel,
        grid_spec=pltpu.PrefetchScalarGridSpec(
            num_scalar_prefetch=1,
            grid=(blocks,),
            in_specs=[
                pl.BlockSpec((row_total, part), lambda t, p: (0, t)),
                pl.BlockSpec((1, slots), lambda t, p: (0, 0)),
                pl.BlockSpec((1, slots, part), lambda t, p: (p[0] ^ t, 0, 0)),
            ],
            out_specs=pl.BlockSpec((row_total, part), lambda t, p: (0, t)),
        ),
        out_shape=jax.ShapeDtypeStruct((row_total, width), jnp.bfloat16),
        cost_estimate=pl.CostEstimate(
            flops=2 * row_total * slots * width, bytes_accessed=4 << 20, transcendentals=0
        ),
        name="stream_rows",
    )(place, residual, token_of_slot, contributions)


def project_pair(place, first, second, token_of_slot, contributions, gain, weights, target):
    blocks, slots, part = contributions.shape
    tok_rows, width = first.shape
    columns = weights.shape[1]
    tile = column_tile(columns)

    def kernel(place_ref, a_ref, b_ref, slots_ref, contributions_ref, gain_ref, w_ref, *rest):
        out, combined, normed = rest[-3:]
        me = place_ref[0]
        owner = place_ref[1]

        @pl.when(pl.program_id(0) == 0)
        def _():
            row = lax.broadcasted_iota(jnp.int32, (tok_rows, slots), 0)
            for h, rows_ref in enumerate((a_ref, b_ref)):
                down = slice(h * tok_rows, (h + 1) * tok_rows)
                table = (row + (owner ^ h) * tok_rows == slots_ref[...]).astype(jnp.bfloat16)
                squares = jnp.zeros((tok_rows, 1), jnp.float32)
                for t in range(blocks):
                    at = slice(t * part, (t + 1) * part)
                    value = rows_ref[:, at].astype(jnp.float32) + jnp.dot(
                        table, contributions_ref[me ^ t], preferred_element_type=jnp.float32
                    )
                    combined[down, at] = value
                    squares = squares + jnp.sum(value * value, axis=1, keepdims=True)
                scale = lax.rsqrt(squares / width + 1e-06)
                for t in range(blocks):
                    at = slice(t * part, (t + 1) * part)
                    normed[down, at] = (combined[down, at] * scale * gain_ref[:, at]).astype(
                        jnp.bfloat16
                    )

        value = jnp.dot(normed[...], w_ref[...], preferred_element_type=jnp.float32)
        value = value.astype(jnp.bfloat16)
        odd = owner % 2
        out[odd] = value[:tok_rows]
        out[1 - odd] = value[tok_rows:]

    in_specs = [
        pl.BlockSpec((tok_rows, width), lambda n, p: (0, 0)),
        pl.BlockSpec((tok_rows, width), lambda n, p: (0, 0)),
        pl.BlockSpec((1, slots), lambda n, p: (0, 0)),
        pl.BlockSpec((blocks, slots, part), lambda n, p: (0, 0, 0)),
        pl.BlockSpec((1, width), lambda n, p: (0, 0)),
        pl.BlockSpec((width, tile), lambda n, p: (0, n)),
    ]
    operands = [place, first, second, token_of_slot, contributions, gain, weights]
    aliases = {}
    if target is not None:
        in_specs.append(pl.BlockSpec(memory_space=pl.ANY))
        operands.append(target)
        aliases = {7: 0}
    return pl.pallas_call(
        kernel,
        grid_spec=pltpu.PrefetchScalarGridSpec(
            num_scalar_prefetch=1,
            grid=(columns // tile,),
            in_specs=in_specs,
            out_specs=pl.BlockSpec((2, tok_rows, tile), lambda n, p: (p[1] // 2, 0, n)),
            scratch_shapes=[
                pltpu.VMEM((2 * tok_rows, width), jnp.float32),
                pltpu.VMEM((2 * tok_rows, width), jnp.bfloat16),
            ],
        ),
        out_shape=jax.ShapeDtypeStruct((blocks, tok_rows, columns), jnp.bfloat16),
        input_output_aliases=aliases,
        cost_estimate=pl.CostEstimate(
            flops=4 * tok_rows * width * (columns + slots),
            bytes_accessed=2 * width * columns,
            transcendentals=0,
        ),
        compiler_params=pltpu.CompilerParams(vmem_limit_bytes=58 << 20),
        name="project_rows",
    )(*operands)


def from_partner(value, count, apart):
    return lax.ppermute(value, "tensor", [(d, d ^ apart) for d in range(count)])


def gather_pairs(value, count):
    pairs = []
    for k in range(0, count, 2):
        near = value if k == 0 else from_partner(value, count, k)
        pairs.append((near, from_partner(near, count, 1)))
    return pairs


def layer(
    expert_inputs, gates, chosen_tokens, w_gate, w_up, w_down, residual, norm_gain, w_qkv
):
    expert_count = lax.axis_size("expert")
    tensor_count = lax.axis_size("tensor")
    group_index = lax.axis_index("expert")
    tensor_index = lax.axis_index("tensor")
    local_experts, slot_count, feature_width = expert_inputs.shape
    tok_rows = residual.shape[0]
    group_rows = tok_rows * tensor_count
    total_experts = expert_count * local_experts
    local_rows = local_experts * slot_count
    feature_part = feature_width // tensor_count

    gathered = gather_pairs(residual, tensor_count)

    in_group = (chosen_tokens // group_rows) == group_index
    rank = jnp.cumsum(in_group.astype(jnp.int32), axis=1) - 1
    per_expert = min(MOST * tensor_count, slot_count)
    compact_rows = total_experts * per_expert
    slot = jnp.where(
        in_group,
        jnp.arange(total_experts, dtype=jnp.int32)[:, None] * per_expert + rank,
        compact_rows,
    ).reshape(-1)
    pick = jnp.arange(compact_rows, dtype=jnp.int32)[:, None] == slot[None, :]
    local_token = (chosen_tokens % group_rows).reshape(-1)
    token_of_slot = jnp.sum(jnp.where(pick, local_token[None, :] + 1, 0), axis=1) - 1
    pick = pick.astype(jnp.bfloat16)

    gate_part = jnp.einsum(
        "ecd,edf->ecf", expert_inputs, w_gate, preferred_element_type=jnp.float32
    )
    up_part = jnp.einsum("ecd,edf->ecf", expert_inputs, w_up, preferred_element_type=jnp.float32)
    hidden = (jax.nn.silu(gate_part) * up_part).astype(jnp.bfloat16)
    partial_value = (
        jnp.einsum("ecf,efd->ecd", hidden, w_down, preferred_element_type=jnp.float32)
        * gates[:, :, None]
    ).astype(jnp.bfloat16)
    partial_rows = partial_value.reshape(local_rows, feature_width)

    blocks = lax.all_to_all(
        partial_rows, "tensor", split_axis=1, concat_axis=0, tiled=True
    ).reshape(tensor_count, local_rows, feature_part)
    summed = lax.optimization_barrier(jnp.sum(blocks.astype(jnp.float32), axis=0))
    every_row = lax.all_gather(summed.astype(jnp.bfloat16), "expert", axis=0, tiled=True)
    compact = jnp.dot(pick, every_row, preferred_element_type=jnp.float32).astype(jnp.bfloat16)
    shared = [piece for pair in gather_pairs(compact, tensor_count) for piece in pair]
    contributions = jnp.stack(shared)

    slots = token_of_slot.reshape(1, compact_rows)
    gain = norm_gain.reshape(1, feature_width)
    me = tensor_index.astype(jnp.int32)
    stream = make_stream(residual, me.reshape(1), slots, contributions)
    projected = None
    for k in range(0, tensor_count, 2):
        place = jnp.stack([me, me ^ k])
        projected = project_pair(
            place, *gathered[k // 2], slots, contributions, gain, w_qkv, projected
        )
    return (stream, projected.reshape(group_rows, -1))


def solution(mesh):
    return jax.shard_map(
        layer,
        mesh=mesh,
        in_specs=(
            P("expert", None, None),
            P("expert", None),
            P(),
            P("expert", None, "tensor"),
            P("expert", None, "tensor"),
            P("expert", "tensor", None),
            P(("expert", "tensor"), None),
            P(),
            P(None, "tensor"),
        ),
        out_specs=(P(("expert", "tensor"), None), P("expert", "tensor")),
        check_vma=False,
    )
```
